32 devices in a mesh: fsdp: 8 (over y, x, core), expert: 4 (over z).
Axes of the slice: x: 2, y: 2, z: 4, core: 2. Of those that a mesh axis runs over, the one named last changes fastest.
Arguments:
- pool: bfloat16 [64, 128, 4096], P('fsdp', None, 'expert'), may hold values from -6 to 6
- picks: int32 [8, 4], P('fsdp'), may hold values from 0 to 7, as said below
- lengths: int32 [64], P('fsdp'), may hold values from 1 to 128
- routes: int32 [4096, 2], P(('fsdp', 'expert')), may hold values from 0 to 7, all different within a row; in each aligned block of 128 rows (0 to 127, 128 to 255, ...) at most 64 rows name the same one
- route_gap: float32 [4096], P(('fsdp', 'expert')), may hold values from -8 to 8
- gate_weight: bfloat16 [8, 14336, 4096], P('expert', 'fsdp'), may hold values from -0.09375 to 0.09375
- down_weight: bfloat16 [8, 14336, 4096], P('expert', 'fsdp'), may hold values from -0.046875 to 0.046875
Outputs:
- moe_out: bfloat16 [4096, 4096], P(('fsdp', 'expert'))
The draws below stay inside these ranges and needn't reach their ends.
Inputs may be any that keep to these rules, and one draw needn't show every extreme that they name: `picks`: each row holds 4 different candidate numbers. `routes`: the two experts of a token differ; among the 128 tokens of one window no expert is named by more than 64 tokens.
All inputs are finite; a program needn't handle non-finite values.
Results may differ from the reference program's by a relative error of at most 0.019.
Values may be sent and summed in bfloat16 or wider, within the bound.
A program may use at most 128 MiB of HBM per device.

```python
import math
import jax
import jax.numpy as jnp
import numpy as np
from jax import lax

D = 4096
EXPERTS = 8
FF_WIN = 14336
TOP = 2
WIN = 128
CAP = 14
MOST = 64
SEL = 4
CAND = 8
POOL = 64
NUM_WIN = 32
TOKENS = 4096
N_FSDP = 8


def draw_picks(key, part):
    row_keys = jax.random.split(jax.random.fold_in(key, 11), N_FSDP)

    def one_row(row_key):
        return jax.random.permutation(row_key, CAND)[:SEL]
    return jax.vmap(one_row)(row_keys).astype(jnp.int32)


def set_ends(drawn, key, least, high):
    spot = [jax.random.randint(jax.random.fold_in(key, axis), (), 0, length) for axis, length in enumerate(drawn.shape)]
    longest = drawn.shape.index(max(drawn.shape))
    next_to = spot[:longest] + [(spot[longest] + 1) % drawn.shape[longest]] + spot[longest + 1:]
    return drawn.at[tuple(spot)].set(least).at[tuple(next_to)].set(high)


def steps_of(rng, shape, cuts, least, largest):
    factor_of = 1.0
    for dim, blocks in cuts:
        draws = jax.random.uniform(jax.random.fold_in(jax.random.fold_in(rng, 6), dim), (blocks,), jnp.float32, least / len(cuts), largest / len(cuts))
        factor_of = factor_of * jnp.repeat(jnp.exp(draws), shape[dim] // blocks).reshape((-1,) + (1,) * (len(shape) - 1 - dim))
    return factor_of


def deal_out(stream_key, own, number, rows, amount, top, bound, lean):
    order = jax.random.permutation(stream_key, amount)
    heavy_load, usual = shares(amount, rows * top, bound, lean, True), shares(amount, rows * top, bound, lean, False)
    places = jnp.arange(amount)

    def named(sizes, offset_by):
        used = int((sizes > 0).sum())
        fixed = max(1, used // 4)
        moved = fixed + (places - fixed + offset_by * (used - fixed)) % max(1, amount - fixed)
        return jnp.zeros((amount,), jnp.int32).at[order[jnp.where(places < fixed, places, moved)]].set(jnp.asarray(sizes, jnp.int32))

    sizes = jnp.where(number % 4 == 0, named(heavy_load, number // 4), named(usual, number - number // 4 - 1))
    mixed = jax.random.permutation(jax.random.fold_in(own, 3), amount)
    source_of, taker = mixed[0:amount // 2 * 2:2], mixed[1:amount // 2 * 2:2]
    margin = jnp.minimum(sizes[source_of] - 1, bound - sizes[taker]) // 2
    margin = jnp.where((source_of == order[0]) | (taker == order[0]) | (sizes[taker] == 0), 0, jnp.maximum(margin, 0))
    moved = jax.random.randint(jax.random.fold_in(own, 4), (amount // 2,), 0, 1 << 20) % (margin + 1)
    sizes = sizes.at[source_of].add(-moved).at[taker].add(moved)
    members = jnp.searchsorted(jnp.cumsum(sizes), jnp.arange(rows * top), side="right").astype(jnp.int32)
    grid = members.reshape(top, rows).T
    grid = grid[jax.random.permutation(jax.random.fold_in(own, 1), rows)]
    offset_by = jax.random.randint(jax.random.fold_in(own, 2), (rows, 1), 0, top)
    return jnp.take_along_axis(grid, (jnp.arange(top)[None, :] + offset_by) % top, axis=1)


def shares(count, total, limit, skew, full):
    weights = [(1 << 20) // math.isqrt(rank ** skew) + 1 for rank in range(1, count + 1)]
    largest = limit if full else min(limit, max(-(-total // count), total * weights[0] // sum(weights)))
    least = 1 if total - largest >= count - 1 else 0
    holding, rest = [largest] + [least] * (count - 1), total - largest - least * (count - 1)
    while rest > 0:
        candidates = [i for i in range(1, count) if holding[i] < largest] or [i for i in range(1, count) if holding[i] < limit]
        whole, left = sum([weights[i] for i in candidates]), rest
        for i in candidates:
            more = min(limit - holding[i], max(1, left * weights[i] // whole), rest)
            holding[i] = holding[i] + more
            rest = rest - more
    return np.array(holding)


def scatter_about(rng, shape, deviation, bound, cuts=(), kind=jnp.bfloat16):
    drawn = deviation * jax.random.normal(rng, shape, jnp.float32)
    if cuts:
        drawn = drawn * steps_of(rng, shape, cuts, -0.22, 0.18)
    return jnp.clip(drawn, -bound, bound).astype(kind)


def setup_inputs(seed: int = 0) -> dict:
    streams_of = jax.random.split(jax.random.key(seed), 8)
    pool = scatter_about(streams_of[0], (POOL, WIN, D), 1.0, 6.0, ((0, 8), (2, 4)))
    picks = draw_picks(jax.random.fold_in(streams_of[7], 71), 0)
    lengths = set_ends(jax.random.randint(streams_of[2], (POOL,), 1, WIN + 1), jax.random.fold_in(streams_of[2], 1), 1, WIN).astype(jnp.int32)
    routes_keys = jax.random.split(jax.random.fold_in(streams_of[3], 1), TOKENS // WIN)
    routes_turns = jax.random.permutation(jax.random.fold_in(streams_of[3], 3), TOKENS // WIN)
    routes = jax.vmap(lambda own, number: deal_out(jax.random.fold_in(streams_of[3], 2), own, number, WIN, EXPERTS, TOP, MOST, 2))(routes_keys, routes_turns).reshape((TOKENS, TOP))
    route_gap = scatter_about(streams_of[4], (TOKENS,), 2.0, 8.0, ((0, 32),), jnp.float32)
    gate_weight = scatter_about(streams_of[5], (EXPERTS, FF_WIN, D), D ** -0.5, 0.09375, ((0, 4), (1, 8)))
    down_weight = scatter_about(streams_of[6], (EXPERTS, FF_WIN, D), FF_WIN ** -0.5, 0.046875, ((0, 4), (1, 8)))
    return dict(pool=pool, picks=picks, lengths=lengths, routes=routes, route_gap=route_gap, gate_weight=gate_weight, down_weight=down_weight)


def slot_targets(block_routes, length):
    row_count = block_routes.shape[0]
    is_live = jnp.arange(row_count, dtype=jnp.int32) < length
    expert_ids = jnp.concatenate([block_routes[:, 0], block_routes[:, 1]])
    live_both = jnp.concatenate([is_live, is_live])
    expert_hits = ((expert_ids[:, None] == jnp.arange(EXPERTS, dtype=jnp.int32)[None, :]) & live_both[:, None]).astype(jnp.int32)
    earlier = jnp.cumsum(expert_hits, axis=0) - expert_hits
    slot_rank = jnp.sum(earlier * expert_hits, axis=1)
    is_kept = live_both & (slot_rank < CAP)
    return jnp.where(is_kept, expert_ids * CAP + slot_rank, -1).astype(jnp.int32)


def dispatch_table(targets):
    row_count = targets.shape[0] // 2
    slot_ids = jnp.arange(EXPERTS * CAP, dtype=jnp.int32)[:, None]
    return ((slot_ids == targets[None, :row_count]) | (slot_ids == targets[None, row_count:])).astype(jnp.float32)


def combine_table(targets, gap_row):
    row_count = targets.shape[0] // 2
    slot_ids = jnp.arange(EXPERTS * CAP, dtype=jnp.int32)[None, :]
    weight_first = jax.nn.sigmoid(gap_row)[:, None]
    weight_second = jax.nn.sigmoid(-gap_row)[:, None]
    first_hit = (targets[:row_count, None] == slot_ids).astype(jnp.float32)
    second_hit = (targets[row_count:, None] == slot_ids).astype(jnp.float32)
    return first_hit * weight_first + second_hit * weight_second


def run_expert(operands):
    slot_rows, gate_matrix, down_matrix = operands
    gate_act = lax.dot_general(slot_rows, gate_matrix, (((1,), (1,)), ((), ())), preferred_element_type=jnp.float32)
    hidden = jax.nn.silu(gate_act).astype(jnp.bfloat16)
    hidden_block = FF_WIN // N_FSDP
    summed = jnp.zeros((slot_rows.shape[0], D), jnp.float32)
    for shard_number in range(N_FSDP):
        lower = shard_number * hidden_block
        partial_value = jnp.dot(hidden[:, lower:lower + hidden_block], down_matrix[lower:lower + hidden_block], preferred_element_type=jnp.float32)
        partial_value = lax.optimization_barrier(partial_value.astype(jnp.bfloat16))
        summed = summed + partial_value.astype(jnp.float32)
    return summed.astype(jnp.bfloat16)


def reference(pool, picks, lengths, routes, route_gap, gate_weight, down_weight):
    shard_base = jnp.arange(N_FSDP, dtype=jnp.int32)[:, None] * CAND
    chosen = (picks + shard_base).reshape(-1).astype(jnp.int32)
    windows = jnp.take(pool, chosen, axis=0)
    window_len = jnp.take(lengths, chosen)
    route_blocks = routes.reshape(NUM_WIN, WIN, TOP)
    gap_rows = route_gap.reshape(NUM_WIN, WIN)
    targets = jax.vmap(slot_targets)(route_blocks, window_len)
    dispatch = jax.vmap(dispatch_table)(targets)
    slot_rows = jnp.einsum("wsp,wpd->wsd", dispatch, windows.astype(jnp.float32), precision=lax.Precision.HIGHEST).astype(jnp.bfloat16)
    slot_rows = slot_rows.reshape(NUM_WIN, EXPERTS, CAP, D).transpose(1, 0, 2, 3).reshape(EXPERTS, NUM_WIN * CAP, D)
    outputs = lax.map(run_expert, (slot_rows, gate_weight, down_weight))
    outputs = outputs.reshape(EXPERTS, NUM_WIN, CAP, D).transpose(1, 0, 2, 3).reshape(NUM_WIN, EXPERTS * CAP, D)
    combine = jax.vmap(combine_table)(targets, gap_rows)
    mixed = jnp.einsum("wps,wsd->wpd", combine, outputs.astype(jnp.float32), precision=lax.Precision.HIGHEST)
    return mixed.reshape(TOKENS, D).astype(jnp.bfloat16)
```

```python
import jax
import jax.numpy as jnp
from jax import lax
from jax.sharding import PartitionSpec as P

EXPERTS = 8
TOP = 2
CAP = 14


def slot_targets(routes, lengths):
    row_count = routes.shape[2]
    is_live = jnp.arange(row_count, dtype=jnp.int32)[None, :] < lengths[:, None]
    expert_ids = jnp.concatenate([routes[:, 0], routes[:, 1]], axis=1)
    live_both = jnp.concatenate([is_live, is_live], axis=1)
    expert_hits = (
        expert_ids[:, None, :] == jnp.arange(EXPERTS, dtype=jnp.int32)[None, :, None]
    ) & live_both[:, None, :]
    entry = jnp.arange(TOP * row_count, dtype=jnp.int32)
    before = (entry[:, None] < entry[None, :]).astype(jnp.bfloat16)
    earlier = jnp.einsum(
        "bej,ji->bei", expert_hits.astype(jnp.bfloat16), before, preferred_element_type=jnp.float32
    )
    slot_rank = jnp.sum(jnp.where(expert_hits, earlier, 0.0), axis=1).astype(jnp.int32)
    is_kept = live_both & (slot_rank < CAP)
    return jnp.where(is_kept, expert_ids * CAP + slot_rank, -1)


def local(pool, picks, lengths, routes, route_gap, gate_weight, down_weight):
    columns = lax.axis_size("expert")
    expert_local = gate_weight.shape[0]
    window_rows = pool.shape[1]
    features = pool.shape[2]
    model_width = gate_weight.shape[2]
    slots = EXPERTS * CAP
    mine = lax.axis_index("expert")

    def shifted(value, step):
        if step == 0:
            return value
        return lax.ppermute(value, "expert", [(i, (i + step) % columns) for i in range(columns)])

    chosen = picks[0]
    selected = jnp.take(pool, chosen, axis=0, mode="clip")
    chosen_len = jnp.take(lengths, chosen, mode="clip")
    own_routes = routes.T
    from_steps = jnp.stack([shifted(own_routes, step) for step in range(columns)])
    source_step = (mine - jnp.arange(columns, dtype=jnp.int32)) % columns
    column_routes = jnp.take(from_steps, source_step, axis=0, mode="clip")
    all_targets = slot_targets(column_routes, chosen_len)

    base = jnp.arange(columns, dtype=jnp.int32)[:, None] * slots
    codes = jnp.where(all_targets >= 0, all_targets + base, -1)
    first_code = codes[:, :window_rows].reshape(-1)
    second_code = codes[:, window_rows:].reshape(-1)
    shape = (expert_local, columns, columns, CAP)
    e_id, k_id, b_id, c_id = (lax.broadcasted_iota(jnp.int32, shape, d) for d in range(4))
    row_code = b_id * slots + (((mine + k_id) % columns) * expert_local + e_id) * CAP + c_id
    row_code = row_code.reshape(-1, 1)
    table = ((row_code == first_code[None, :]) | (row_code == second_code[None, :])).astype(
        jnp.bfloat16
    )
    outgoing = jnp.dot(
        table,
        selected.reshape(columns * window_rows, features),
        preferred_element_type=jnp.float32,
    ).astype(jnp.bfloat16)
    block = columns * CAP

    gathered = []
    for e in range(expert_local):
        arrived = jnp.zeros((block, model_width), jnp.bfloat16)
        for step in range(columns):
            start = (e * columns + step) * block
            piece = shifted(outgoing[start : start + block], step)
            arrived = lax.dynamic_update_slice(
                arrived, piece, (0, ((mine - step) % columns) * features)
            )
        gathered.append(lax.all_gather(arrived, "fsdp", axis=0, tiled=True))

    summed = []
    for e in range(expert_local):
        gate_act = lax.dot_general(
            gathered[e],
            gate_weight[e],
            (((1,), (1,)), ((), ())),
            preferred_element_type=jnp.float32,
        )
        hidden = jax.nn.silu(gate_act).astype(jnp.bfloat16)
        partial_value = jnp.dot(
            hidden, down_weight[e], preferred_element_type=jnp.float32
        ).astype(jnp.bfloat16)
        summed.append(lax.psum_scatter(partial_value, "fsdp", scatter_dimension=0, tiled=True))

    my_targets = lax.dynamic_index_in_dim(all_targets, mine, 0, keepdims=False)
    weight_first = jax.nn.sigmoid(route_gap)[:, None]
    weight_second = jax.nn.sigmoid(-route_gap)[:, None]
    mixed = jnp.zeros((window_rows, model_width), jnp.float32)
    for e in range(expert_local):
        pieces = []
        for step in range(columns):
            piece = lax.dynamic_slice_in_dim(
                summed[e], ((mine + step) % columns) * CAP, CAP, axis=0
            )
            pieces.append(shifted(piece, step))
        returned = jnp.concatenate(pieces, axis=0).astype(jnp.float32)
        k_id = lax.broadcasted_iota(jnp.int32, (columns, CAP), 0)
        c_id = lax.broadcasted_iota(jnp.int32, (columns, CAP), 1)
        slot_ids = ((((mine - k_id) % columns) * expert_local + e) * CAP + c_id).reshape(1, -1)
        first_hit = (my_targets[:window_rows, None] == slot_ids).astype(jnp.float32)
        second_hit = (my_targets[window_rows:, None] == slot_ids).astype(jnp.float32)
        combine = first_hit * weight_first + second_hit * weight_second
        mixed = mixed + jnp.dot(
            combine, returned, precision=lax.Precision.HIGHEST, preferred_element_type=jnp.float32
        )
    return mixed.astype(jnp.bfloat16)


def solution(mesh):
    placed = (
        P("fsdp", None, "expert"),
        P("fsdp", None),
        P("fsdp"),
        P(("fsdp", "expert"), None),
        P(("fsdp", "expert")),
        P("expert", "fsdp", None),
        P("expert", "fsdp", None),
    )
    return jax.shard_map(
        local, mesh=mesh, in_specs=placed, out_specs=P(("fsdp", "expert"), None), check_vma=False
    )
```
